32 devices in a mesh: region: 8 (over y, x, core), member: 4 (over z).
Axes of the slice: x: 2, y: 2, z: 4, core: 2. Of those that a mesh axis runs over, the one named last changes fastest.
Arguments:
- controls: float32 [16, 8, 128, 512], P('member', None, 'region'), may hold values from -6 to 6
- perturbations: float32 [64, 8, 128, 512], P('member', None, 'region'), may hold values from -1.5 to 1.5
- assignment: int32 [64], replicated, may hold values from 0 to 15
- courant: float32 [4, 4, 8, 128, 512], P(None, None, 'member', 'region'), may hold values from 0.02 to 0.24
- innovation: float32 [8, 128, 512], P('member', 'region'), may hold values from -6 to 6
- obs_weight: float32 [8, 128, 512], P('member', 'region'), may hold values from 0.3 to 3
Outputs:
- gradient: float32 [16, 8, 128, 512], P('member', None, 'region')
- departure: float32 [8, 128, 512], P('member', 'region')
The draws below stay inside these ranges and needn't reach their ends.
All inputs are finite; a program needn't handle non-finite values.
Results may differ from the reference program's by a relative error of at most 0.0001.
Values sent between devices are 32-bit elements; how exact they have to be, the bound alone decides.
No kernel may reach another device: no remote copies, remote signals or barrier semaphores. Data moves between devices by JAX's collectives and lax.ppermute only.
A program may use at most 64 MiB of HBM per device.

```python
import math
import jax
import jax.numpy as jnp
from jax import lax

NY = 512
NZ = 8
FIELDS = 16
MEMBERS = 64
PASSES = 16
STEPS = 4
NX = 128


def place_ends(result, stream_key, smallest, high):
    extent = result.shape
    index_at = [jax.random.randint(jax.random.fold_in(stream_key, axis), (), 0, extent[axis]) for axis in range(len(extent))]
    result = result.at[tuple(index_at)].set(smallest)
    longest = extent.index(max(extent))
    index_at[longest] = (index_at[longest] + 1) % extent[longest]
    return result.at[tuple(index_at)].set(high)


def block_scale(rng, extent, pieces, smallest, top_value):
    def one(dim, shards_of):
        draws = jax.random.uniform(jax.random.fold_in(jax.random.fold_in(rng, 6), dim), (shards_of,), jnp.float32, smallest / len(pieces), top_value / len(pieces))
        return jnp.repeat(jnp.exp(draws), extent[dim] // shards_of).reshape((-1,) + (1,) * (len(extent) - dim - 1))

    gain = one(*pieces[0])
    for cut in pieces[1:]:
        gain = gain * one(*cut)
    return gain


def centred(rng, extent, spread, bound, cuts=(), held_as=jnp.bfloat16):
    drawn = jax.random.normal(rng, extent, jnp.float32) * spread
    if len(cuts) > 0:
        drawn = block_scale(rng, extent, cuts, -0.22, 0.18) * drawn
    return jnp.clip(drawn, min=-bound, max=bound).astype(held_as)


def setup_inputs(seed: int = 0) -> dict:
    splits = jax.random.split(jax.random.key(seed), 7)
    controls = centred(splits[0], (FIELDS, NZ, NX, NY), 1.0, 6.0, ((0, 4), (2, 8)), jnp.float32)
    perturbations = centred(splits[1], (MEMBERS, NZ, NX, NY), 0.25, 1.5, ((0, 4), (2, 8)), jnp.float32)
    assignment = place_ends(jax.random.randint(splits[2], (MEMBERS,), 0, FIELDS), jax.random.fold_in(splits[2], 1), 0, FIELDS - 1).astype(jnp.int32)
    courant = jnp.clip(0.02 + 0.22 * jax.random.uniform(splits[3], (STEPS, 4, NZ, NX, NY), jnp.float32) ** block_scale(splits[3], (STEPS, 4, NZ, NX, NY), ((2, 4), (3, 8)), -0.2, 0.2), 0.02, 0.24)
    innovation = centred(splits[4], (NZ, NX, NY), 1.0, 6.0, ((0, 4), (1, 8)), jnp.float32)
    obs_weight = jnp.clip(jnp.exp(math.log(3.0) - 2.3025851 * jax.random.uniform(splits[5], (NZ, NX, NY), jnp.float32) ** block_scale(splits[5], (NZ, NX, NY), ((0, 4), (1, 8)), -0.2, 0.2)), 0.3, 3.0)
    return dict(controls=controls, perturbations=perturbations, assignment=assignment, courant=courant, innovation=innovation, obs_weight=obs_weight)


def smooth(fields):
    for repeat in range(PASSES):
        padded = jnp.pad(fields, ((0, 0), (0, 0), (1, 1), (1, 1)))
        beside_all = padded[:, :, 2:, 1:-1] + padded[:, :, :-2, 1:-1] + padded[:, :, 1:-1, 2:] + padded[:, :, 1:-1, :-2]
        fields = fields + 0.2 * (beside_all - 4.0 * fields)
    return fields

def transport(state, courant):
    for step in range(STEPS):
        coeffs = courant[step]
        padded = jnp.pad(state, ((0, 0), (1, 1), (1, 1)))
        center = 1.0 - lax.optimization_barrier(jnp.sum(coeffs, 0))
        state = center * state + coeffs[0] * padded[:, :-2, 1:-1] + coeffs[1] * padded[:, 2:, 1:-1] + coeffs[2] * padded[:, 1:-1, :-2] + coeffs[3] * padded[:, 1:-1, 2:]
    return state

def reference(controls, perturbations, assignment, courant, innovation, obs_weight):
    one_hot = (assignment[:, None] == jnp.arange(FIELDS, dtype=jnp.int32)[None, :]).astype(jnp.float32)
    smoothed = smooth(controls)
    member_sums = jnp.einsum('kl,kzxy->lzxy', one_hot, perturbations, precision=lax.Precision.HIGHEST)
    increment = lax.optimization_barrier(jnp.sum(smoothed * member_sums, 0))
    moved, pull_back = jax.vjp(lambda value: transport(value, courant), increment)
    departure = obs_weight * (moved - innovation)
    adjoint = pull_back(departure)[0]
    field_terms = jnp.einsum('kl,kzxy->lzxy', one_hot, perturbations * adjoint[None], precision=lax.Precision.HIGHEST)
    gradient = controls + smooth(field_terms)
    return (gradient, departure)
```

```python
import functools

import jax
import jax.numpy as jnp
import numpy as np
from jax import lax
from jax.experimental import pallas as pl
from jax.experimental.pallas import tpu as pltpu
from jax.sharding import PartitionSpec as P

FIELDS = 16
PASSES = 16
STEPS = 4
RATE = 0.2
STACK = 4
F32 = jnp.float32
BF16 = jnp.bfloat16


def sine_basis(n):
    k = np.arange(1, n + 1, dtype=np.float64)
    return np.sqrt(2.0 / (n + 1)) * np.sin(np.pi * np.outer(k, k) / (n + 1))


def halves(matrix):
    high = np.asarray(matrix, np.float32).astype(jnp.bfloat16)
    low = (np.asarray(matrix, np.float64) - high.astype(np.float64)).astype(jnp.bfloat16)
    return np.stack([high, low])


@functools.lru_cache(None)
def diffusion_tables(rows, cols):
    depth = PASSES
    window = rows + 2 * depth
    col_basis = sine_basis(cols)
    row_basis = sine_basis(window)
    first = np.eye(window)
    first[:depth] = 0.0
    for i in range(depth - 1):
        first[i, depth + depth - 2 - i] = -1.0
    last = np.eye(window)
    last[depth + rows :] = 0.0
    for i in range(1, depth):
        last[depth + rows + i, depth + rows - i] = -1.0
    forward = [row_basis @ first, row_basis, row_basis @ last]
    stacked = np.eye(STACK)
    forward = np.stack([halves(np.kron(stacked, m)) for m in forward])
    backward = halves(np.kron(stacked, row_basis[depth : depth + rows]))
    row_values = 2.0 * np.cos(np.pi * np.arange(1, window + 1) / (window + 1))
    col_values = 2.0 * np.cos(np.pi * np.arange(1, cols + 1) / (cols + 1))
    scale = (RATE * (1.0 + row_values[:, None] + col_values[None, :])) ** PASSES
    return halves(col_basis), forward, backward, scale.astype(np.float32)


def split(x):
    high = x.astype(BF16)
    return high, (x - high.astype(F32)).astype(BF16)


def mul(a, b):
    dot = functools.partial(jnp.dot, preferred_element_type=F32)
    return dot(a[0], b[0]) + (dot(a[1], b[0]) + dot(a[0], b[1]))


def diffuse_block(ext, col_ref, fwd_ref, bwd_ref, scale_ref, rows):
    pairs, window, cols = ext.shape
    col = (col_ref[0], col_ref[1])
    fwd = (fwd_ref[0], fwd_ref[1])
    bwd = (bwd_ref[0], bwd_ref[1])
    spectral = mul(split(ext.reshape(pairs * window, cols)), col)
    group = STACK * window
    outs = []
    for g in range(pairs // STACK):
        part = mul(fwd, split(spectral[g * group : (g + 1) * group]))
        part = (part.reshape(STACK, window, cols) * scale_ref[...][None]).reshape(group, cols)
        outs.append(mul(bwd, split(part)))
    out = mul(split(jnp.concatenate(outs, 0)), col)
    return out.reshape(pairs, rows, cols)


def smooth_kernel(top_ref, own_ref, bot_ref, col_ref, fwd_ref, bwd_ref, scale_ref, out_ref):
    ext = jnp.concatenate([top_ref[0], own_ref[0], bot_ref[0]], axis=1)
    out_ref[0] = diffuse_block(ext, col_ref, fwd_ref, bwd_ref, scale_ref, own_ref.shape[2])


def gradient_kernel(
    slot_ref, ctl_ref, top_ref, own_ref, bot_ref, atop_ref, aown_ref, abot_ref,
    col_ref, fwd_ref, bwd_ref, scale_ref, out_ref,
):
    levels = own_ref.shape[1]
    parts = []
    for z in range(levels):
        s = slot_ref[z]
        parts.append(
            jnp.concatenate(
                [top_ref[0, z] * atop_ref[s], own_ref[0, z] * aown_ref[s], bot_ref[0, z] * abot_ref[s]],
                axis=0,
            )
        )
    ext = jnp.stack(parts)
    out_ref[0] = ctl_ref[0] + diffuse_block(ext, col_ref, fwd_ref, bwd_ref, scale_ref, own_ref.shape[2])


def table_specs(tables):
    def spec(t):
        return pl.BlockSpec(t.shape, functools.partial(lambda n, *_: (0,) * n, t.ndim))

    return [spec(t) for t in tables]


def smooth(top, own, bot, tables):
    fields, levels, rows, cols = own.shape
    block = lambda a: pl.BlockSpec((1,) + a.shape[1:], lambda f: (f, 0, 0, 0))
    return pl.pallas_call(
        smooth_kernel,
        grid=(fields,),
        in_specs=[block(top), block(own), block(bot)] + table_specs(tables),
        out_specs=block(own),
        out_shape=jax.ShapeDtypeStruct(own.shape, F32),
        cost_estimate=pl.CostEstimate(flops=5 * 10**9, bytes_accessed=4 * own.size * 4, transcendentals=0),
        name="smooth",
    )(top, own, bot, *tables)


def gradient_of(slots, controls, sums, adjoints, tables):
    fields, levels, rows, cols = controls.shape
    block = lambda a: pl.BlockSpec((1,) + a.shape[1:], lambda f, s: (f, 0, 0, 0))
    whole = lambda a: pl.BlockSpec(a.shape, lambda f, s: (0, 0, 0))
    return pl.pallas_call(
        gradient_kernel,
        grid_spec=pltpu.PrefetchScalarGridSpec(
            num_scalar_prefetch=1,
            grid=(fields,),
            in_specs=[block(controls)]
            + [block(a) for a in sums]
            + [whole(a) for a in adjoints]
            + table_specs(tables),
            out_specs=block(controls),
        ),
        out_shape=jax.ShapeDtypeStruct(controls.shape, F32),
        cost_estimate=pl.CostEstimate(flops=5 * 10**9, bytes_accessed=5 * controls.size * 4, transcendentals=0),
        name="gradient",
    )(slots, controls, *sums, *adjoints, *tables)


def member_sums_kernel(assign_ref, members_ref, out_ref):
    out_ref[...] = jnp.zeros_like(out_ref)
    for k in range(members_ref.shape[0]):
        field = assign_ref[k]
        out_ref[field] = out_ref[field] + members_ref[k]


def member_sums(assignment, perturbations):
    members, levels, rows, cols = perturbations.shape
    return pl.pallas_call(
        member_sums_kernel,
        grid_spec=pltpu.PrefetchScalarGridSpec(
            num_scalar_prefetch=1,
            grid=(levels,),
            in_specs=[pl.BlockSpec((members, 1, rows, cols), lambda z, s: (0, z, 0, 0))],
            out_specs=pl.BlockSpec((FIELDS, 1, rows, cols), lambda z, s: (0, z, 0, 0)),
        ),
        out_shape=jax.ShapeDtypeStruct((FIELDS, levels, rows, cols), F32),
        cost_estimate=pl.CostEstimate(flops=10**7, bytes_accessed=2 * perturbations.size * 4, transcendentals=0),
        name="member_sums",
    )(assignment, perturbations)


def shift_rows(x, by):
    blank = jnp.zeros_like(x[:, :1])
    if by > 0:
        return jnp.concatenate([blank, x[:, :-1]], axis=1)
    return jnp.concatenate([x[:, 1:], blank], axis=1)


def shift_cols(x, by):
    lane = lax.broadcasted_iota(jnp.int32, x.shape, 2)
    if by > 0:
        return jnp.where(lane == 0, 0.0, pltpu.roll(x, 1, 2))
    return jnp.where(lane == x.shape[2] - 1, 0.0, pltpu.roll(x, x.shape[2] - 1, 2))


def transport_kernel(
    inc_top, inc_own, inc_bot, con_top, con_own, con_bot, obs_own, inn_own, dep_ref, adj_ref
):
    halo = inc_top.shape[1]
    rows = inc_own.shape[1]
    join = lambda a, b, c: jnp.concatenate([a, b, c], axis=1)
    state = join(inc_top[...], inc_own[...], inc_bot[...])

    def coeffs(step):
        c = [
            join(con_top[4 * step + k], con_own[4 * step + k], con_bot[4 * step + k]) for k in range(4)
        ]
        return c, 1.0 - (c[0] + c[1] + c[2] + c[3])

    for step in range(STEPS):
        c, center = coeffs(step)
        state = (
            center * state
            + c[0] * shift_rows(state, 1)
            + c[1] * shift_rows(state, -1)
            + c[2] * shift_cols(state, 1)
            + c[3] * shift_cols(state, -1)
        )
    weight = join(con_top[4 * STEPS], obs_own[...], con_bot[4 * STEPS])
    target = join(con_top[4 * STEPS + 1], inn_own[...], con_bot[4 * STEPS + 1])
    state = weight * (state - target)
    dep_ref[...] = state[:, halo : halo + rows]
    for step in range(STEPS - 1, -1, -1):
        c, center = coeffs(step)
        state = (
            center * state
            + shift_rows(c[0] * state, -1)
            + shift_rows(c[1] * state, 1)
            + shift_cols(c[2] * state, -1)
            + shift_cols(c[3] * state, 1)
        )
    adj_ref[...] = state[:, halo : halo + rows]


def transport(inc, con, obs_weight, innovation):
    shape = jax.ShapeDtypeStruct(obs_weight.shape, F32)
    return pl.pallas_call(
        transport_kernel,
        out_shape=(shape, shape),
        cost_estimate=pl.CostEstimate(flops=10**8, bytes_accessed=3 * 2**20, transcendentals=0),
        name="transport",
    )(*inc, *con, obs_weight, innovation)


def beside(block, dim, depth, axis="region"):
    count = lax.axis_size(axis)
    forward = [(i, i + 1) for i in range(count - 1)]
    backward = [(b, a) for a, b in forward]
    extent = block.shape[dim]
    low = lax.ppermute(lax.slice_in_dim(block, extent - depth, extent, axis=dim), axis, forward)
    high = lax.ppermute(lax.slice_in_dim(block, 0, depth, axis=dim), axis, backward)
    return low, high


def shards(controls, perturbations, assignment, courant, innovation, obs_weight):
    fields, levels, rows, cols = controls.shape
    planes = lax.axis_size("member")
    plane = lax.axis_index("member")
    region = lax.axis_index("region")
    regions = lax.axis_size("region")
    own_levels = levels // planes
    halo = 2 * STEPS

    col_basis, forward, backward, scale = diffusion_tables(rows, cols)
    place = jnp.where(region == 0, 0, jnp.where(region == regions - 1, 2, 1))
    tables = (
        jnp.asarray(col_basis),
        lax.dynamic_index_in_dim(jnp.asarray(forward), place, 0, keepdims=False),
        jnp.asarray(backward),
        jnp.asarray(scale),
    )

    local_members = perturbations.shape[0]
    own_assignment = lax.dynamic_slice_in_dim(assignment, plane * local_members, local_members, 0)
    partial_sums = member_sums(own_assignment, perturbations)
    sums = lax.psum_scatter(partial_sums, "member", scatter_dimension=0, tiled=True)

    top, bot = beside(controls, 2, PASSES)
    flat = courant.reshape((4 * STEPS,) + courant.shape[2:])
    ends = lambda a: jnp.concatenate([a[:, :halo], a[:, rows - halo :]], axis=1)
    edge = jnp.concatenate(
        [
            jnp.concatenate([flat[:, :, :halo], flat[:, :, rows - halo :]], axis=2),
            ends(obs_weight)[None],
            ends(innovation)[None],
        ],
        axis=0,
    )
    con_top, con_bot = beside(edge, 2, halo)
    smoothed = smooth(top, controls, bot, tables)

    partial = jnp.sum(smoothed * sums, 0).reshape(planes, own_levels, rows, cols)
    pick = lambda k: lax.dynamic_index_in_dim(partial, lax.rem(plane + k, planes), 0, keepdims=False)
    turn = lambda k: [(i, (i + k) % planes) for i in range(planes)]
    increment = pick(0)
    for k in range(1, planes):
        increment = increment + lax.ppermute(pick(k), "member", turn(k))
    inc_top, inc_bot = beside(increment, 1, halo)
    sums_top, sums_bot = beside(sums, 2, PASSES)
    departure, adjoint = transport(
        (inc_top, increment, inc_bot), (con_top, flat, con_bot), obs_weight, innovation
    )
    full = jnp.concatenate(
        [adjoint] + [lax.ppermute(adjoint, "member", turn(k)) for k in range(1, planes)], axis=0
    )
    adj_top, adj_bot = beside(full, 1, PASSES)
    level = lax.iota(jnp.int32, levels)
    slots = lax.rem(plane - level // own_levels + planes, planes) * own_levels + lax.rem(level, own_levels)
    gradient = gradient_of(
        slots, controls, (sums_top, sums, sums_bot), (adj_top, full, adj_bot), tables
    )
    return (gradient, departure)


def solution(mesh):
    return jax.shard_map(
        shards,
        mesh=mesh,
        in_specs=(
            P("member", None, "region", None),
            P("member", None, "region", None),
            P(),
            P(None, None, "member", "region", None),
            P("member", "region", None),
            P("member", "region", None),
        ),
        out_specs=(P("member", None, "region", None), P("member", "region", None)),
        check_vma=False,
    )
```

```python
import functools

import jax
import jax.numpy as jnp
import numpy as np
from jax import lax
from jax.experimental import pallas as pl
from jax.experimental.pallas import tpu as pltpu
from jax.sharding import PartitionSpec as P


FIELDS = 16
PASSES = 16
STEPS = 4
RATE = 0.2
STACK = 4
TILE = 8
PARTS = 2
F32 = jnp.float32
BF16 = jnp.bfloat16


def sine_basis(n):
    k = np.arange(1, n + 1, dtype=np.float64)
    return np.sqrt(2.0 / (n + 1)) * np.sin(np.pi * np.outer(k, k) / (n + 1))


def halves(matrix):
    high = np.asarray(matrix, np.float32).astype(jnp.bfloat16)
    low = (np.asarray(matrix, np.float64) - high.astype(np.float64)).astype(jnp.bfloat16)
    return np.stack([high, low])


@functools.lru_cache(None)
def diffusion_tables(rows, cols):
    depth = PASSES
    window = rows + 2 * depth
    col_basis = sine_basis(cols)
    row_basis = sine_basis(window)
    first = np.eye(window)
    first[:depth] = 0.0
    for i in range(depth - 1):
        first[i, depth + depth - 2 - i] = -1.0
    last = np.eye(window)
    last[depth + rows :] = 0.0
    for i in range(1, depth):
        last[depth + rows + i, depth + rows - i] = -1.0
    forward = [row_basis @ first, row_basis, row_basis @ last]
    stacked = np.eye(STACK)
    forward = np.stack([halves(np.kron(stacked, m)) for m in forward])
    backward = halves(np.kron(stacked, row_basis[depth : depth + rows]))
    row_values = 2.0 * np.cos(np.pi * np.arange(1, window + 1) / (window + 1))
    col_values = 2.0 * np.cos(np.pi * np.arange(1, cols + 1) / (cols + 1))
    scale = (RATE * (1.0 + row_values[:, None] + col_values[None, :])) ** PASSES
    return halves(col_basis), forward, backward, scale.astype(np.float32)


def split(x):
    high = x.astype(BF16)
    return high, (x - high.astype(F32)).astype(BF16)


def mul(a, b):
    dot = functools.partial(jnp.dot, preferred_element_type=F32)
    return dot(a[0], b[0]) + (dot(a[1], b[0]) + dot(a[0], b[1]))


def diffuse_block(ext, col_ref, fwd_ref, bwd_ref, scale_ref, rows):
    pairs, window, cols = ext.shape
    col = (col_ref[0], col_ref[1])
    fwd = (fwd_ref[0], fwd_ref[1])
    bwd = (bwd_ref[0], bwd_ref[1])
    spectral = mul(split(ext.reshape(pairs * window, cols)), col)
    group = STACK * window
    outs = []
    for g in range(pairs // STACK):
        part = mul(fwd, split(spectral[g * group : (g + 1) * group]))
        part = (part.reshape(STACK, window, cols) * scale_ref[...][None]).reshape(group, cols)
        outs.append(mul(bwd, split(part)))
    out = mul(split(jnp.concatenate(outs, 0)), col)
    return out.reshape(pairs, rows, cols)


def smooth_kernel(top_ref, own_ref, bot_ref, col_ref, fwd_ref, bwd_ref, scale_ref, out_ref):
    flat = lambda ref, rows: ref[...].reshape(-1, rows, ref.shape[-1])
    ext = jnp.concatenate(
        [flat(top_ref, PASSES), flat(own_ref, own_ref.shape[2]), flat(bot_ref, PASSES)], axis=1
    )
    out = diffuse_block(ext, col_ref, fwd_ref, bwd_ref, scale_ref, own_ref.shape[2])
    out_ref[...] = out.reshape(out_ref.shape)


def gradient_kernel(planes, ctl_ref, *refs):
    sums, adjoints, tables, out_ref = refs[:-8], refs[-8:-5], refs[-5:-1], refs[-1]
    step, levels, rows, _ = ctl_ref.shape
    span = sums[0].shape[1]
    own = levels // planes
    plane = lax.axis_index("member")
    slots = [lax.rem(plane + planes - z // own, planes) * own + z % own for z in range(levels)]
    parts = []
    for f in range(step):
        for z in range(levels):
            blocks = sums[3 * (z // span) : 3 * (z // span) + 3]
            parts.append(
                jnp.concatenate([b[f, z % span] * a[slots[z]] for b, a in zip(blocks, adjoints)], axis=0)
            )
    out = diffuse_block(jnp.stack(parts), *tables, rows)
    out_ref[...] = ctl_ref[...] + out.reshape(out_ref.shape)


def grid_place():
    region, regions = lax.axis_index("region"), lax.axis_size("region")
    return (region > 0).astype(jnp.int32) + (region == regions - 1).astype(jnp.int32)


def table_specs(tables):
    def spec(t):
        if t.ndim == 4:
            return pl.BlockSpec((None,) + t.shape[1:], lambda *_: (grid_place(), 0, 0, 0))
        return pl.BlockSpec(t.shape, functools.partial(lambda n, *_: (0,) * n, t.ndim))

    return [spec(t) for t in tables]


def smooth(top, own, bot, tables):
    fields, levels, _, cols = own.shape
    step = 2 if fields % 2 == 0 else 1
    block = lambda a: pl.BlockSpec((step,) + a.shape[1:], lambda f: (f, 0, 0, 0))
    halo = pl.BlockSpec((step * levels * PASSES // TILE, TILE, cols), lambda f: (f, 0, 0))
    return pl.pallas_call(
        smooth_kernel,
        grid=(fields // step,),
        in_specs=[halo, block(own), halo] + table_specs(tables),
        out_specs=block(own),
        out_shape=jax.ShapeDtypeStruct(own.shape, F32),
        cost_estimate=pl.CostEstimate(flops=5 * 10**9, bytes_accessed=4 * own.size * 4, transcendentals=0),
        name="smooth",
    )(top, own, bot, *tables)


def gradient_of(planes, controls, sums, adjoints, tables):
    fields, _, _, _ = controls.shape
    step = 2 if fields % 2 == 0 else 1
    block = lambda a: pl.BlockSpec((step,) + a.shape[1:], lambda f: (f, 0, 0, 0))
    return pl.pallas_call(
        functools.partial(gradient_kernel, planes),
        grid=(fields // step,),
        in_specs=[block(controls)]
        + [block(a) for a in sums]
        + table_specs(adjoints)
        + table_specs(tables),
        out_specs=block(controls),
        out_shape=jax.ShapeDtypeStruct(controls.shape, F32),
        cost_estimate=pl.CostEstimate(flops=5 * 10**9, bytes_accessed=5 * controls.size * 4, transcendentals=0),
        name="gradient",
    )(controls, *sums, *adjoints, *tables)


def member_sums_kernel(assign_ref, members_ref, out_ref, last_ref, first_ref):
    members = members_ref.shape[0]
    offset = lax.axis_index("member") * members
    out_ref[...] = jnp.zeros_like(out_ref)
    for k in range(members):
        field = assign_ref[offset + k]
        out_ref[field] = out_ref[field] + members_ref[k]
    fields = first_ref.shape[0]
    last_ref[...] = out_ref[out_ref.shape[0] - fields :]
    first_ref[...] = out_ref[:fields]


def member_sums(assignment, perturbations, part, levels, fields):
    members, _, rows, cols = perturbations.shape
    step = 2 if levels % 2 == 0 else 1
    start = part * levels // step
    spec = lambda n: pl.BlockSpec((n, step, rows, cols), lambda z, s: (0, z, 0, 0))
    shape = lambda n: jax.ShapeDtypeStruct((n, levels, rows, cols), F32)
    return pl.pallas_call(
        member_sums_kernel,
        grid_spec=pltpu.PrefetchScalarGridSpec(
            num_scalar_prefetch=1,
            grid=(levels // step,),
            in_specs=[pl.BlockSpec((members, step, rows, cols), lambda z, s: (0, z + start, 0, 0))],
            out_specs=(spec(FIELDS), spec(fields), spec(fields)),
        ),
        out_shape=(shape(FIELDS), shape(fields), shape(fields)),
        cost_estimate=pl.CostEstimate(flops=10**7, bytes_accessed=perturbations.size * 4, transcendentals=0),
        name="member_sums",
    )(assignment, perturbations)


def forward_kernel(index_ref, rise_ref, fall_ref, up_ref, down_ref, rise_out, fall_out):
    rise_out[...] = rise_ref[...] + up_ref[...]
    fall_out[...] = fall_ref[...] + down_ref[...]


def block_spec(shape, which):
    return pl.BlockSpec(shape, lambda i, s: (s[which],) + (0,) * (len(shape) - 1))


def whole_spec(shape):
    return pl.BlockSpec(shape, lambda i, s: (0,) * len(shape))


def forward_sums(index, partial_sums, up, down):
    spec = whole_spec(up.shape)
    return pl.pallas_call(
        forward_kernel,
        grid_spec=pltpu.PrefetchScalarGridSpec(
            num_scalar_prefetch=1,
            grid=(1,),
            in_specs=[block_spec(up.shape, 0), block_spec(up.shape, 1), spec, spec],
            out_specs=(spec, spec),
        ),
        out_shape=(jax.ShapeDtypeStruct(up.shape, F32),) * 2,
        cost_estimate=pl.CostEstimate(flops=10**6, bytes_accessed=6 * up.size * 4, transcendentals=0),
        name="forward_sums",
    )(index, partial_sums, partial_sums, up, down)


def finish_kernel(planes, index_ref, field_ref, *refs):
    parts, sums, outs, joined = refs[: 3 * PARTS], refs[3 * PARTS : 4 * PARTS], refs[4 * PARTS : -1], refs[-1]
    span = parts[0].shape[1]
    for p in range(PARTS):
        own, up, down = parts[3 * p : 3 * p + 3]
        levels = slice(p * span, (p + 1) * span)
        term = None
        for f in range(own.shape[0]):
            total = own[f] + up[f] + down[f]
            sums[p][f] = total
            term = field_ref[f, levels] * total if term is None else term + field_ref[f, levels] * total
        joined[levels] = term
    own_levels = outs[0].shape[0]
    plane = lax.axis_index("member")
    for k, out in enumerate(outs):
        start = lax.rem(plane + k, planes) * own_levels
        for z in range(own_levels):
            out[z] = joined[start + z]


def finish_sums(index, partial_sums, up, down, smoothed, planes):
    _, levels, rows, cols = smoothed.shape
    spec = whole_spec(up[0].shape)
    out_shapes = [u.shape for u in up] + [(levels // planes, rows, cols)] * planes
    operands, specs = [smoothed], [whole_spec(smoothed.shape)]
    for p in range(PARTS):
        operands += [partial_sums[p], up[p], down[p]]
        specs += [block_spec(up[p].shape, 0), spec, spec]
    return pl.pallas_call(
        functools.partial(finish_kernel, planes),
        grid_spec=pltpu.PrefetchScalarGridSpec(
            num_scalar_prefetch=1,
            grid=(1,),
            in_specs=specs,
            out_specs=[whole_spec(o) for o in out_shapes],
            scratch_shapes=[pltpu.VMEM((levels, rows, cols), F32)],
        ),
        out_shape=[jax.ShapeDtypeStruct(o, F32) for o in out_shapes],
        cost_estimate=pl.CostEstimate(flops=10**6, bytes_accessed=5 * smoothed.size * 4, transcendentals=0),
        name="finish_sums",
    )(index, *operands)


def shift_rows(x, by):
    blank = jnp.zeros_like(x[:, :1])
    if by > 0:
        return jnp.concatenate([blank, x[:, :-1]], axis=1)
    return jnp.concatenate([x[:, 1:], blank], axis=1)


def shift_cols(x, by):
    lane = lax.broadcasted_iota(jnp.int32, x.shape, 2)
    if by > 0:
        return jnp.where(lane == 0, 0.0, pltpu.roll(x, 1, 2))
    return jnp.where(lane == x.shape[2] - 1, 0.0, pltpu.roll(x, x.shape[2] - 1, 2))


def transport_kernel(
    inc_top, inc_own, inc_bot, top_ref, con_own, bot_ref, obs_own, inn_own, dep_ref, adj_ref
):
    halo = inc_top.shape[1]
    con_top, con_bot = [r[...].reshape((-1,) + inc_top.shape) for r in (top_ref, bot_ref)]
    rows = inc_own.shape[1]
    join = lambda a, b, c: jnp.concatenate([a, b, c], axis=1)
    state = join(inc_top[...], inc_own[...], inc_bot[...])

    def coeffs(step):
        c = [
            join(con_top[4 * step + k], con_own[4 * step + k], con_bot[4 * step + k]) for k in range(4)
        ]
        return c, 1.0 - (c[0] + c[1] + c[2] + c[3])

    for step in range(STEPS):
        c, center = coeffs(step)
        state = (
            center * state
            + c[0] * shift_rows(state, 1)
            + c[1] * shift_rows(state, -1)
            + c[2] * shift_cols(state, 1)
            + c[3] * shift_cols(state, -1)
        )
    weight = join(con_top[4 * STEPS], obs_own[...], con_bot[4 * STEPS])
    target = join(con_top[4 * STEPS + 1], inn_own[...], con_bot[4 * STEPS + 1])
    state = weight * (state - target)
    dep_ref[...] = state[:, halo : halo + rows]
    for step in range(STEPS - 1, -1, -1):
        c, center = coeffs(step)
        state = (
            center * state
            + shift_rows(c[0] * state, -1)
            + shift_rows(c[1] * state, 1)
            + shift_cols(c[2] * state, -1)
            + shift_cols(c[3] * state, 1)
        )
    adj_ref[...] = state[:, halo : halo + rows]


def transport(inc, con, obs_weight, innovation, used):
    shape = jax.ShapeDtypeStruct(obs_weight.shape, F32)
    whole = lambda a: pl.BlockSpec(a.shape, lambda i: (0,) * a.ndim)
    tail = con[0].shape[0] - used
    part = pl.BlockSpec(
        (pl.Element(tail), pl.Element(con[0].shape[1]), pl.Element(con[0].shape[2])), lambda i: (used, 0, 0)
    )
    return pl.pallas_call(
        transport_kernel,
        grid=(1,),
        in_specs=[whole(a) for a in inc] + [part, whole(con[1]), part, whole(obs_weight), whole(innovation)],
        out_specs=(whole(obs_weight), whole(obs_weight)),
        out_shape=(shape, shape),
        cost_estimate=pl.CostEstimate(flops=10**8, bytes_accessed=3 * 2**20, transcendentals=0),
        name="transport",
    )(*inc, *con, obs_weight, innovation)


def beside(block, dim, depth, axis="region"):
    count = lax.axis_size(axis)
    forward = [(i, i + 1) for i in range(count - 1)]
    backward = [(b, a) for a, b in forward]
    extent = block.shape[dim]
    low = lax.ppermute(lax.slice_in_dim(block, extent - depth, extent, axis=dim), axis, forward)
    high = lax.ppermute(lax.slice_in_dim(block, 0, depth, axis=dim), axis, backward)
    return low, high


def shards(controls, perturbations, assignment, courant, innovation, obs_weight):
    fields, levels, rows, cols = controls.shape
    planes = lax.axis_size("member")
    plane = lax.axis_index("member")
    regions = lax.axis_size("region")
    halo = 2 * STEPS

    col_basis, forward, backward, scale = diffusion_tables(rows, cols)
    tables = (
        jnp.asarray(col_basis),
        jnp.asarray(forward),
        jnp.asarray(backward),
        jnp.asarray(scale),
    )

    span = levels // PARTS
    partial_sums = [member_sums(assignment, perturbations, p, span, fields) for p in range(PARTS)]

    flat = courant.reshape((4 * STEPS,) + courant.shape[2:])

    def message(low):
        cut = lambda a, dim, depth: lax.slice_in_dim(
            a, *((0, depth) if low else (rows - depth, rows)), axis=dim
        )
        edge = [cut(flat, 2, halo), cut(obs_weight, 1, halo)[None], cut(innovation, 1, halo)[None]]
        return jnp.concatenate(
            [cut(controls, 2, PASSES).reshape(-1, TILE, cols)] + [e.reshape(-1, TILE, cols) for e in edge]
        )

    ahead = [(i, i + 1) for i in range(regions - 1)]
    top = lax.ppermute(message(False), "region", ahead)
    bot = lax.ppermute(message(True), "region", [(j, i) for i, j in ahead])
    used = fields * levels * PASSES // TILE
    smoothed = smooth(top, controls, bot, tables)

    up = [None] * PARTS
    down = [None] * PARTS
    for t in range(planes - 1):
        targets = jnp.clip(
            jnp.stack([plane + (planes - 1) - t, plane - (planes - 1) + t]), 0, planes - 1
        )
        for p in range(PARTS):
            whole, rise, fall = partial_sums[p]
            if t > 0:
                rise, fall = forward_sums(targets, whole, up[p], down[p])
            up[p] = lax.ppermute(rise, "member", [(i, i + 1) for i in range(t + 1)])
            down[p] = lax.ppermute(
                fall, "member", [(planes - 1 - i, planes - 2 - i) for i in range(t + 1)]
            )
    finished = finish_sums(
        plane[None], [whole for whole, _, _ in partial_sums], up, down, smoothed, planes
    )
    sums, partial = finished[:PARTS], finished[PARTS:]
    turn = lambda k: [(i, (i + k) % planes) for i in range(planes)]
    increment = partial[0]
    for k in range(1, planes):
        increment = increment + lax.ppermute(partial[k], "member", turn(k))
    inc_top, inc_bot = beside(increment, 1, halo)
    sums_ext = []
    for p in range(PARTS):
        sums_top, sums_bot = beside(sums[p], 2, PASSES)
        sums_ext += [sums_top, sums[p], sums_bot]
    departure, adjoint = transport(
        (inc_top, increment, inc_bot), (top, flat, bot), obs_weight, innovation, used
    )
    full = jnp.concatenate(
        [adjoint] + [lax.ppermute(adjoint, "member", turn(k)) for k in range(1, planes)], axis=0
    )
    adj_top, adj_bot = beside(full, 1, PASSES)
    gradient = gradient_of(planes, controls, sums_ext, (adj_top, full, adj_bot), tables)
    return (gradient, departure)


def solution(mesh):
    return jax.shard_map(
        shards,
        mesh=mesh,
        in_specs=(
            P("member", None, "region", None),
            P("member", None, "region", None),
            P(),
            P(None, None, "member", "region", None),
            P("member", "region", None),
            P("member", "region", None),
        ),
        out_specs=(P("member", None, "region", None), P("member", "region", None)),
        check_vma=False,
    )
```

```python
import functools

import jax
import jax.numpy as jnp
import numpy as np
from jax import lax
from jax.experimental import pallas as pl
from jax.experimental.pallas import tpu as pltpu
from jax.sharding import PartitionSpec as P


FIELDS = 16
PASSES = 16
STEPS = 4
RATE = 0.2
STACK = 4
TILE = 8
MIB = 2**20
PARTS = 2
F32 = jnp.float32
BF16 = jnp.bfloat16


def sine_basis(n):
    k = np.arange(1, n + 1, dtype=np.float64)
    return np.sqrt(2.0 / (n + 1)) * np.sin(np.pi * np.outer(k, k) / (n + 1))


def halves(matrix):
    high = np.asarray(matrix, np.float32).astype(jnp.bfloat16)
    low = (np.asarray(matrix, np.float64) - high.astype(np.float64)).astype(jnp.bfloat16)
    return np.stack([high, low])


@functools.lru_cache(None)
def diffusion_tables(rows, cols):
    depth = PASSES
    window = rows + 2 * depth
    col_basis = sine_basis(cols)
    row_basis = sine_basis(window)
    first = np.eye(window)
    first[:depth] = 0.0
    for i in range(depth - 1):
        first[i, depth + depth - 2 - i] = -1.0
    last = np.eye(window)
    last[depth + rows :] = 0.0
    for i in range(1, depth):
        last[depth + rows + i, depth + rows - i] = -1.0
    forward = [row_basis @ first, row_basis, row_basis @ last]
    stacked = np.eye(STACK)
    forward = np.stack([halves(np.kron(stacked, m)) for m in forward])
    backward = halves(np.kron(stacked, row_basis[depth : depth + rows]))
    row_values = 2.0 * np.cos(np.pi * np.arange(1, window + 1) / (window + 1))
    col_values = 2.0 * np.cos(np.pi * np.arange(1, cols + 1) / (cols + 1))
    scale = (RATE * (1.0 + row_values[:, None] + col_values[None, :])) ** PASSES
    return halves(col_basis), forward, backward, scale.astype(np.float32)


def split(x):
    high = x.astype(BF16)
    return high, (x - high.astype(F32)).astype(BF16)


def mul(a, b):
    dot = functools.partial(jnp.dot, preferred_element_type=F32)
    return dot(a[0], b[0]) + (dot(a[1], b[0]) + dot(a[0], b[1]))


def diffuse_block(ext, col_ref, fwd_ref, bwd_ref, scale_ref, rows):
    pairs, window, cols = ext.shape
    col = (col_ref[0], col_ref[1])
    fwd = (fwd_ref[0], fwd_ref[1])
    bwd = (bwd_ref[0], bwd_ref[1])
    spectral = mul(split(ext.reshape(pairs * window, cols)), col)
    group = STACK * window
    outs = []
    for g in range(pairs // STACK):
        part = mul(fwd, split(spectral[g * group : (g + 1) * group]))
        part = (part.reshape(STACK, window, cols) * scale_ref[...][None]).reshape(group, cols)
        outs.append(mul(bwd, split(part)))
    out = mul(split(jnp.concatenate(outs, 0)), col)
    return out.reshape(pairs, rows, cols)


def smooth_kernel(top_ref, own_ref, bot_ref, col_ref, fwd_ref, bwd_ref, scale_ref, out_ref):
    flat = lambda ref, rows: ref[...].reshape(-1, rows, ref.shape[-1])
    ext = jnp.concatenate(
        [flat(top_ref, PASSES), flat(own_ref, own_ref.shape[2]), flat(bot_ref, PASSES)], axis=1
    )
    out = diffuse_block(ext, col_ref, fwd_ref, bwd_ref, scale_ref, own_ref.shape[2])
    out_ref[...] = out.reshape(out_ref.shape)


def gradient_kernel(planes, ctl_ref, *refs):
    sums, adjoints, tables, out_ref = refs[:-8], refs[-8:-5], refs[-5:-1], refs[-1]
    step, levels, rows, _ = ctl_ref.shape
    span = sums[0].shape[1]
    own = levels // planes
    plane = lax.axis_index("member")
    slots = [lax.rem(plane + planes - z // own, planes) * own + z % own for z in range(levels)]
    parts = []
    for f in range(step):
        for z in range(levels):
            blocks = sums[3 * (z // span) : 3 * (z // span) + 3]
            parts.append(
                jnp.concatenate([b[f, z % span] * a[slots[z]] for b, a in zip(blocks, adjoints)], axis=0)
            )
    out = diffuse_block(jnp.stack(parts), *tables, rows)
    out_ref[...] = ctl_ref[...] + out.reshape(out_ref.shape)


def grid_place():
    region, regions = lax.axis_index("region"), lax.axis_size("region")
    return (region > 0).astype(jnp.int32) + (region == regions - 1).astype(jnp.int32)


def table_specs(tables):
    def spec(t):
        if t.ndim == 4:
            return pl.BlockSpec((None,) + t.shape[1:], lambda *_: (grid_place(), 0, 0, 0))
        return pl.BlockSpec(t.shape, functools.partial(lambda n, *_: (0,) * n, t.ndim))

    return [spec(t) for t in tables]


def smooth(top, own, bot, tables):
    fields, levels, _, cols = own.shape
    step = 2 if fields % 2 == 0 else 1
    block = lambda a: pl.BlockSpec((step,) + a.shape[1:], lambda f: (f, 0, 0, 0))
    halo = pl.BlockSpec((step * levels * PASSES // TILE, TILE, cols), lambda f: (f, 0, 0))
    return pl.pallas_call(
        smooth_kernel,
        grid=(fields // step,),
        in_specs=[halo, block(own), halo] + table_specs(tables),
        out_specs=block(own),
        out_shape=jax.ShapeDtypeStruct(own.shape, F32),
        cost_estimate=pl.CostEstimate(flops=5 * 10**9, bytes_accessed=4 * own.size * 4, transcendentals=0),
        name="smooth",
        compiler_params=pltpu.CompilerParams(vmem_limit_bytes=20 * MIB),
    )(top, own, bot, *tables)


def gradient_of(planes, controls, sums, adjoints, tables):
    fields, _, _, _ = controls.shape
    step = 2 if fields % 2 == 0 else 1
    block = lambda a: pl.BlockSpec((step,) + a.shape[1:], lambda f: (f, 0, 0, 0))
    return pl.pallas_call(
        functools.partial(gradient_kernel, planes),
        grid=(fields // step,),
        in_specs=[block(controls)]
        + [block(a) for a in sums]
        + table_specs(adjoints)
        + table_specs(tables),
        out_specs=block(controls),
        out_shape=jax.ShapeDtypeStruct(controls.shape, F32),
        cost_estimate=pl.CostEstimate(flops=5 * 10**9, bytes_accessed=5 * controls.size * 4, transcendentals=0),
        name="gradient",
        compiler_params=pltpu.CompilerParams(vmem_limit_bytes=24 * MIB),
    )(controls, *sums, *adjoints, *tables)


def member_sums_kernel(assign_ref, members_ref, out_ref, last_ref, first_ref):
    members = members_ref.shape[0]
    offset = lax.axis_index("member") * members
    out_ref[...] = jnp.zeros_like(out_ref)
    for k in range(members):
        field = assign_ref[offset + k]
        out_ref[field] = out_ref[field] + members_ref[k]
    fields = first_ref.shape[0]
    last_ref[...] = out_ref[out_ref.shape[0] - fields :]
    first_ref[...] = out_ref[:fields]


def member_sums(assignment, perturbations, part, levels, fields):
    members, _, rows, cols = perturbations.shape
    step = 2 if levels % 2 == 0 else 1
    start = part * levels // step
    spec = lambda n: pl.BlockSpec((n, step, rows, cols), lambda z, s: (0, z, 0, 0))
    shape = lambda n: jax.ShapeDtypeStruct((n, levels, rows, cols), F32)
    return pl.pallas_call(
        member_sums_kernel,
        grid_spec=pltpu.PrefetchScalarGridSpec(
            num_scalar_prefetch=1,
            grid=(levels // step,),
            in_specs=[pl.BlockSpec((members, step, rows, cols), lambda z, s: (0, z + start, 0, 0))],
            out_specs=(spec(FIELDS), spec(fields), spec(fields)),
        ),
        out_shape=(shape(FIELDS), shape(fields), shape(fields)),
        cost_estimate=pl.CostEstimate(flops=10**7, bytes_accessed=perturbations.size * 4, transcendentals=0),
        name="member_sums",
    )(assignment, perturbations)


def forward_kernel(index_ref, rise_ref, fall_ref, up_ref, down_ref, rise_out, fall_out):
    rise_out[...] = rise_ref[...] + up_ref[...]
    fall_out[...] = fall_ref[...] + down_ref[...]


def block_spec(shape, which):
    return pl.BlockSpec(shape, lambda i, s: (s[which],) + (0,) * (len(shape) - 1))


def whole_spec(shape):
    return pl.BlockSpec(shape, lambda i, s: (0,) * len(shape))


def forward_sums(index, partial_sums, up, down):
    spec = whole_spec(up.shape)
    return pl.pallas_call(
        forward_kernel,
        grid_spec=pltpu.PrefetchScalarGridSpec(
            num_scalar_prefetch=1,
            grid=(1,),
            in_specs=[block_spec(up.shape, 0), block_spec(up.shape, 1), spec, spec],
            out_specs=(spec, spec),
        ),
        out_shape=(jax.ShapeDtypeStruct(up.shape, F32),) * 2,
        cost_estimate=pl.CostEstimate(flops=10**6, bytes_accessed=6 * up.size * 4, transcendentals=0),
        name="forward_sums",
        compiler_params=pltpu.CompilerParams(vmem_limit_bytes=14 * MIB),
    )(index, partial_sums, partial_sums, up, down)


def finish_kernel(planes, index_ref, field_ref, *refs):
    parts, sums, outs, joined = refs[: 3 * PARTS], refs[3 * PARTS : 4 * PARTS], refs[4 * PARTS : -1], refs[-1]
    span = parts[0].shape[1]
    for p in range(PARTS):
        own, up, down = parts[3 * p : 3 * p + 3]
        levels = slice(p * span, (p + 1) * span)
        term = None
        for f in range(own.shape[0]):
            total = own[f] + up[f] + down[f]
            sums[p][f] = total
            term = field_ref[f, levels] * total if term is None else term + field_ref[f, levels] * total
        joined[levels] = term
    own_levels = outs[0].shape[0]
    plane = lax.axis_index("member")
    for k, out in enumerate(outs):
        start = lax.rem(plane + k, planes) * own_levels
        for z in range(own_levels):
            out[z] = joined[start + z]


def finish_sums(index, partial_sums, up, down, smoothed, planes):
    _, levels, rows, cols = smoothed.shape
    spec = whole_spec(up[0].shape)
    out_shapes = [u.shape for u in up] + [(levels // planes, rows, cols)] * planes
    operands, specs = [smoothed], [whole_spec(smoothed.shape)]
    for p in range(PARTS):
        operands += [partial_sums[p], up[p], down[p]]
        specs += [block_spec(up[p].shape, 0), spec, spec]
    return pl.pallas_call(
        functools.partial(finish_kernel, planes),
        grid_spec=pltpu.PrefetchScalarGridSpec(
            num_scalar_prefetch=1,
            grid=(1,),
            in_specs=specs,
            out_specs=[whole_spec(o) for o in out_shapes],
            scratch_shapes=[pltpu.VMEM((levels, rows, cols), F32)],
        ),
        out_shape=[jax.ShapeDtypeStruct(o, F32) for o in out_shapes],
        cost_estimate=pl.CostEstimate(flops=10**6, bytes_accessed=5 * smoothed.size * 4, transcendentals=0),
        name="finish_sums",
        compiler_params=pltpu.CompilerParams(vmem_limit_bytes=16 * MIB),
    )(index, *operands)


def shift_rows(x, by):
    blank = jnp.zeros_like(x[:, :1])
    if by > 0:
        return jnp.concatenate([blank, x[:, :-1]], axis=1)
    return jnp.concatenate([x[:, 1:], blank], axis=1)


def shift_cols(x, by):
    lane = lax.broadcasted_iota(jnp.int32, x.shape, 2)
    if by > 0:
        return jnp.where(lane == 0, 0.0, pltpu.roll(x, 1, 2))
    return jnp.where(lane == x.shape[2] - 1, 0.0, pltpu.roll(x, x.shape[2] - 1, 2))


def transport_kernel(
    inc_top, inc_own, inc_bot, top_ref, con_own, bot_ref, obs_own, inn_own, dep_ref, adj_ref
):
    halo = inc_top.shape[1]
    con_top, con_bot = [r[...].reshape((-1,) + inc_top.shape) for r in (top_ref, bot_ref)]
    rows = inc_own.shape[1]
    join = lambda a, b, c: jnp.concatenate([a, b, c], axis=1)
    state = join(inc_top[...], inc_own[...], inc_bot[...])

    def coeffs(step):
        c = [
            join(con_top[4 * step + k], con_own[4 * step + k], con_bot[4 * step + k]) for k in range(4)
        ]
        return c, 1.0 - (c[0] + c[1] + c[2] + c[3])

    for step in range(STEPS):
        c, center = coeffs(step)
        state = (
            center * state
            + c[0] * shift_rows(state, 1)
            + c[1] * shift_rows(state, -1)
            + c[2] * shift_cols(state, 1)
            + c[3] * shift_cols(state, -1)
        )
    weight = join(con_top[4 * STEPS], obs_own[...], con_bot[4 * STEPS])
    target = join(con_top[4 * STEPS + 1], inn_own[...], con_bot[4 * STEPS + 1])
    state = weight * (state - target)
    dep_ref[...] = state[:, halo : halo + rows]
    for step in range(STEPS - 1, -1, -1):
        c, center = coeffs(step)
        state = (
            center * state
            + shift_rows(c[0] * state, -1)
            + shift_rows(c[1] * state, 1)
            + shift_cols(c[2] * state, -1)
            + shift_cols(c[3] * state, 1)
        )
    adj_ref[...] = state[:, halo : halo + rows]


def transport(inc, con, obs_weight, innovation, used):
    shape = jax.ShapeDtypeStruct(obs_weight.shape, F32)
    whole = lambda a: pl.BlockSpec(a.shape, lambda i: (0,) * a.ndim)
    tail = con[0].shape[0] - used
    part = pl.BlockSpec(
        (pl.Element(tail), pl.Element(con[0].shape[1]), pl.Element(con[0].shape[2])), lambda i: (used, 0, 0)
    )
    return pl.pallas_call(
        transport_kernel,
        grid=(1,),
        in_specs=[whole(a) for a in inc] + [part, whole(con[1]), part, whole(obs_weight), whole(innovation)],
        out_specs=(whole(obs_weight), whole(obs_weight)),
        out_shape=(shape, shape),
        cost_estimate=pl.CostEstimate(flops=10**8, bytes_accessed=3 * 2**20, transcendentals=0),
        name="transport",
        compiler_params=pltpu.CompilerParams(vmem_limit_bytes=16 * MIB),
    )(*inc, *con, obs_weight, innovation)


def beside(block, dim, depth, axis="region"):
    count = lax.axis_size(axis)
    forward = [(i, i + 1) for i in range(count - 1)]
    backward = [(b, a) for a, b in forward]
    extent = block.shape[dim]
    low = lax.ppermute(lax.slice_in_dim(block, extent - depth, extent, axis=dim), axis, forward)
    high = lax.ppermute(lax.slice_in_dim(block, 0, depth, axis=dim), axis, backward)
    return low, high


def shards(controls, perturbations, assignment, courant, innovation, obs_weight):
    fields, levels, rows, cols = controls.shape
    planes = lax.axis_size("member")
    plane = lax.axis_index("member")
    regions = lax.axis_size("region")
    halo = 2 * STEPS

    col_basis, forward, backward, scale = diffusion_tables(rows, cols)
    tables = (
        jnp.asarray(col_basis),
        jnp.asarray(forward),
        jnp.asarray(backward),
        jnp.asarray(scale),
    )

    span = levels // PARTS
    partial_sums = [member_sums(assignment, perturbations, p, span, fields) for p in range(PARTS)]

    flat = courant.reshape((4 * STEPS,) + courant.shape[2:])

    def message(low):
        cut = lambda a, dim, depth: lax.slice_in_dim(
            a, *((0, depth) if low else (rows - depth, rows)), axis=dim
        )
        edge = [cut(flat, 2, halo), cut(obs_weight, 1, halo)[None], cut(innovation, 1, halo)[None]]
        return jnp.concatenate(
            [cut(controls, 2, PASSES).reshape(-1, TILE, cols)] + [e.reshape(-1, TILE, cols) for e in edge]
        )

    ahead = [(i, i + 1) for i in range(regions - 1)]
    top = lax.ppermute(message(False), "region", ahead)
    bot = lax.ppermute(message(True), "region", [(j, i) for i, j in ahead])
    used = fields * levels * PASSES // TILE
    smoothed = smooth(top, controls, bot, tables)

    up = [None] * PARTS
    down = [None] * PARTS
    for t in range(planes - 1):
        targets = jnp.clip(
            jnp.stack([plane + (planes - 1) - t, plane - (planes - 1) + t]), 0, planes - 1
        )
        for p in range(PARTS):
            whole, rise, fall = partial_sums[p]
            if t > 0:
                rise, fall = forward_sums(targets, whole, up[p], down[p])
            up[p] = lax.ppermute(rise, "member", [(i, i + 1) for i in range(t + 1)])
            down[p] = lax.ppermute(
                fall, "member", [(planes - 1 - i, planes - 2 - i) for i in range(t + 1)]
            )
    finished = finish_sums(
        plane[None], [whole for whole, _, _ in partial_sums], up, down, smoothed, planes
    )
    sums, partial = finished[:PARTS], finished[PARTS:]
    turn = lambda k: [(i, (i + k) % planes) for i in range(planes)]
    increment = partial[0]
    for k in range(1, planes):
        increment = increment + lax.ppermute(partial[k], "member", turn(k))
    inc_top, inc_bot = beside(increment, 1, halo)
    sums_ext = []
    for p in range(PARTS):
        sums_top, sums_bot = beside(sums[p], 2, PASSES)
        sums_ext += [sums_top, sums[p], sums_bot]
    departure, adjoint = transport(
        (inc_top, increment, inc_bot), (top, flat, bot), obs_weight, innovation, used
    )
    full = jnp.concatenate(
        [adjoint] + [lax.ppermute(adjoint, "member", turn(k)) for k in range(1, planes)], axis=0
    )
    adj_top, adj_bot = beside(full, 1, PASSES)
    gradient = gradient_of(planes, controls, sums_ext, (adj_top, full, adj_bot), tables)
    return (gradient, departure)


def solution(mesh):
    return jax.shard_map(
        shards,
        mesh=mesh,
        in_specs=(
            P("member", None, "region", None),
            P("member", None, "region", None),
            P(),
            P(None, None, "member", "region", None),
            P("member", "region", None),
            P("member", "region", None),
        ),
        out_specs=(P("member", None, "region", None), P("member", "region", None)),
        check_vma=False,
    )
```

```python
import functools

import jax
import jax.numpy as jnp
import numpy as np
from jax import lax
from jax.experimental import pallas as pl
from jax.experimental.pallas import tpu as pltpu
from jax.sharding import PartitionSpec as P


FIELDS = 16
PASSES = 16
STEPS = 4
RATE = 0.2
STACK = 4
TILE = 8
MIB = 2**20
PARTS = 2
F32 = jnp.float32
BF16 = jnp.bfloat16


def sine_basis(n):
    k = np.arange(1, n + 1, dtype=np.float64)
    return np.sqrt(2.0 / (n + 1)) * np.sin(np.pi * np.outer(k, k) / (n + 1))


def halves(matrix):
    high = np.asarray(matrix, np.float32).astype(jnp.bfloat16)
    low = (np.asarray(matrix, np.float64) - high.astype(np.float64)).astype(jnp.bfloat16)
    return np.stack([high, low])


@functools.lru_cache(None)
def diffusion_tables(rows, cols):
    depth = PASSES
    window = rows + 2 * depth
    col_basis = sine_basis(cols)
    row_basis = sine_basis(window)
    first = np.eye(window)
    first[:depth] = 0.0
    for i in range(depth - 1):
        first[i, depth + depth - 2 - i] = -1.0
    last = np.eye(window)
    last[depth + rows :] = 0.0
    for i in range(1, depth):
        last[depth + rows + i, depth + rows - i] = -1.0
    forward = [row_basis @ first, row_basis, row_basis @ last]
    stacked = np.eye(STACK)
    forward = np.stack([halves(np.kron(stacked, m)) for m in forward])
    backward = halves(np.kron(stacked, row_basis[depth : depth + rows]))
    row_values = 2.0 * np.cos(np.pi * np.arange(1, window + 1) / (window + 1))
    col_values = 2.0 * np.cos(np.pi * np.arange(1, cols + 1) / (cols + 1))
    scale = (RATE * (1.0 + row_values[:, None] + col_values[None, :])) ** PASSES
    return halves(col_basis), forward, backward, scale.astype(np.float32)


def split(x):
    high = x.astype(BF16)
    return high, (x - high.astype(F32)).astype(BF16)


def mul(a, b):
    dot = functools.partial(jnp.dot, preferred_element_type=F32)
    return dot(a[0], b[0]) + (dot(a[1], b[0]) + dot(a[0], b[1]))


def diffuse_block(ext, col_ref, fwd_ref, bwd_ref, scale_ref, rows):
    pairs, window, cols = ext.shape
    col = (col_ref[0], col_ref[1])
    fwd = (fwd_ref[0], fwd_ref[1])
    bwd = (bwd_ref[0], bwd_ref[1])
    spectral = mul(split(ext.reshape(pairs * window, cols)), col)
    group = STACK * window
    outs = []
    for g in range(pairs // STACK):
        part = mul(fwd, split(spectral[g * group : (g + 1) * group]))
        part = (part.reshape(STACK, window, cols) * scale_ref[...][None]).reshape(group, cols)
        outs.append(mul(bwd, split(part)))
    out = mul(split(jnp.concatenate(outs, 0)), col)
    return out.reshape(pairs, rows, cols)


def smooth_kernel(top_ref, own_ref, bot_ref, col_ref, fwd_ref, bwd_ref, scale_ref, out_ref):
    flat = lambda ref, rows: ref[...].reshape(-1, rows, ref.shape[-1])
    ext = jnp.concatenate(
        [flat(top_ref, PASSES), flat(own_ref, own_ref.shape[2]), flat(bot_ref, PASSES)], axis=1
    )
    out = diffuse_block(ext, col_ref, fwd_ref, bwd_ref, scale_ref, own_ref.shape[2])
    out_ref[...] = out.reshape(out_ref.shape)


def gradient_kernel(planes, ctl_ref, *refs):
    sums, adjoints, tables, out_ref = refs[:-8], refs[-8:-5], refs[-5:-1], refs[-1]
    step, levels, rows, _ = ctl_ref.shape
    span = sums[0].shape[1]
    own = levels // planes
    plane = lax.axis_index("member")
    slots = [lax.rem(plane + planes - z // own, planes) * own + z % own for z in range(levels)]
    parts = []
    for f in range(step):
        for z in range(levels):
            blocks = sums[3 * (z // span) : 3 * (z // span) + 3]
            parts.append(
                jnp.concatenate([b[f, z % span] * a[slots[z]] for b, a in zip(blocks, adjoints)], axis=0)
            )
    out = diffuse_block(jnp.stack(parts), *tables, rows)
    out_ref[...] = ctl_ref[...] + out.reshape(out_ref.shape)


def grid_place():
    region, regions = lax.axis_index("region"), lax.axis_size("region")
    return (region > 0).astype(jnp.int32) + (region == regions - 1).astype(jnp.int32)


def table_specs(tables):
    def spec(t):
        if t.ndim == 4:
            return pl.BlockSpec((None,) + t.shape[1:], lambda *_: (grid_place(), 0, 0, 0))
        return pl.BlockSpec(t.shape, functools.partial(lambda n, *_: (0,) * n, t.ndim))

    return [spec(t) for t in tables]


def smooth(top, own, bot, tables):
    fields, levels, _, cols = own.shape
    step = 2 if fields % 2 == 0 else 1
    block = lambda a: pl.BlockSpec((step,) + a.shape[1:], lambda f: (f, 0, 0, 0))
    halo = pl.BlockSpec((step * levels * PASSES // TILE, TILE, cols), lambda f: (f, 0, 0))
    return pl.pallas_call(
        smooth_kernel,
        grid=(fields // step,),
        in_specs=[halo, block(own), halo] + table_specs(tables),
        out_specs=block(own),
        out_shape=jax.ShapeDtypeStruct(own.shape, F32),
        cost_estimate=pl.CostEstimate(flops=5 * 10**9, bytes_accessed=4 * own.size * 4, transcendentals=0),
        name="smooth",
        compiler_params=pltpu.CompilerParams(vmem_limit_bytes=20 * MIB),
    )(top, own, bot, *tables)


def gradient_of(planes, controls, sums, adjoints, tables):
    fields, _, _, _ = controls.shape
    step = fields
    block = lambda a: pl.BlockSpec((step,) + a.shape[1:], lambda f: (f, 0, 0, 0))
    return pl.pallas_call(
        functools.partial(gradient_kernel, planes),
        grid=(fields // step,),
        in_specs=[block(controls)]
        + [block(a) for a in sums]
        + table_specs(adjoints)
        + table_specs(tables),
        out_specs=block(controls),
        out_shape=jax.ShapeDtypeStruct(controls.shape, F32),
        cost_estimate=pl.CostEstimate(flops=5 * 10**9, bytes_accessed=5 * controls.size * 4, transcendentals=0),
        name="gradient",
        compiler_params=pltpu.CompilerParams(vmem_limit_bytes=24 * MIB),
    )(controls, *sums, *adjoints, *tables)


def member_sums_kernel(assign_ref, members_ref, out_ref, last_ref, first_ref):
    members = members_ref.shape[0]
    offset = lax.axis_index("member") * members
    out_ref[...] = jnp.zeros_like(out_ref)
    for k in range(members):
        field = assign_ref[offset + k]
        out_ref[field] = out_ref[field] + members_ref[k]
    fields = first_ref.shape[0]
    last_ref[...] = out_ref[out_ref.shape[0] - fields :]
    first_ref[...] = out_ref[:fields]


def member_sums(assignment, perturbations, part, levels, fields):
    members, _, rows, cols = perturbations.shape
    step = 2 if levels % 2 == 0 else 1
    start = part * levels // step
    spec = lambda n: pl.BlockSpec((n, step, rows, cols), lambda z, s: (0, z, 0, 0))
    shape = lambda n: jax.ShapeDtypeStruct((n, levels, rows, cols), F32)
    return pl.pallas_call(
        member_sums_kernel,
        grid_spec=pltpu.PrefetchScalarGridSpec(
            num_scalar_prefetch=1,
            grid=(levels // step,),
            in_specs=[pl.BlockSpec((members, step, rows, cols), lambda z, s: (0, z + start, 0, 0))],
            out_specs=(spec(FIELDS), spec(fields), spec(fields)),
        ),
        out_shape=(shape(FIELDS), shape(fields), shape(fields)),
        cost_estimate=pl.CostEstimate(flops=10**7, bytes_accessed=perturbations.size * 4, transcendentals=0),
        name="member_sums",
    )(assignment, perturbations)


def forward_kernel(index_ref, rise_ref, fall_ref, up_ref, down_ref, rise_out, fall_out):
    rise_out[...] = rise_ref[...] + up_ref[...]
    fall_out[...] = fall_ref[...] + down_ref[...]


def block_spec(shape, which):
    return pl.BlockSpec(shape, lambda i, s: (s[which],) + (0,) * (len(shape) - 1))


def whole_spec(shape):
    return pl.BlockSpec(shape, lambda i, s: (0,) * len(shape))


def forward_sums(index, partial_sums, up, down):
    spec = whole_spec(up.shape)
    return pl.pallas_call(
        forward_kernel,
        grid_spec=pltpu.PrefetchScalarGridSpec(
            num_scalar_prefetch=1,
            grid=(1,),
            in_specs=[block_spec(up.shape, 0), block_spec(up.shape, 1), spec, spec],
            out_specs=(spec, spec),
        ),
        out_shape=(jax.ShapeDtypeStruct(up.shape, F32),) * 2,
        cost_estimate=pl.CostEstimate(flops=10**6, bytes_accessed=6 * up.size * 4, transcendentals=0),
        name="forward_sums",
        compiler_params=pltpu.CompilerParams(vmem_limit_bytes=14 * MIB),
    )(index, partial_sums, partial_sums, up, down)


def finish_kernel(planes, index_ref, field_ref, *refs):
    parts, sums, outs, joined = refs[: 3 * PARTS], refs[3 * PARTS : 4 * PARTS], refs[4 * PARTS : -1], refs[-1]
    span = parts[0].shape[1]
    for p in range(PARTS):
        own, up, down = parts[3 * p : 3 * p + 3]
        levels = slice(p * span, (p + 1) * span)
        term = None
        for f in range(own.shape[0]):
            total = own[f] + up[f] + down[f]
            sums[p][f] = total
            term = field_ref[f, levels] * total if term is None else term + field_ref[f, levels] * total
        joined[levels] = term
    own_levels = outs[0].shape[0]
    plane = lax.axis_index("member")
    for k, out in enumerate(outs):
        start = lax.rem(plane + k, planes) * own_levels
        for z in range(own_levels):
            out[z] = joined[start + z]


def finish_sums(index, partial_sums, up, down, smoothed, planes):
    _, levels, rows, cols = smoothed.shape
    spec = whole_spec(up[0].shape)
    out_shapes = [u.shape for u in up] + [(levels // planes, rows, cols)] * planes
    operands, specs = [smoothed], [whole_spec(smoothed.shape)]
    for p in range(PARTS):
        operands += [partial_sums[p], up[p], down[p]]
        specs += [block_spec(up[p].shape, 0), spec, spec]
    return pl.pallas_call(
        functools.partial(finish_kernel, planes),
        grid_spec=pltpu.PrefetchScalarGridSpec(
            num_scalar_prefetch=1,
            grid=(1,),
            in_specs=specs,
            out_specs=[whole_spec(o) for o in out_shapes],
            scratch_shapes=[pltpu.VMEM((levels, rows, cols), F32)],
        ),
        out_shape=[jax.ShapeDtypeStruct(o, F32) for o in out_shapes],
        cost_estimate=pl.CostEstimate(flops=10**6, bytes_accessed=5 * smoothed.size * 4, transcendentals=0),
        name="finish_sums",
        compiler_params=pltpu.CompilerParams(vmem_limit_bytes=16 * MIB),
    )(index, *operands)


def shift_rows(x, by):
    blank = jnp.zeros_like(x[:, :1])
    if by > 0:
        return jnp.concatenate([blank, x[:, :-1]], axis=1)
    return jnp.concatenate([x[:, 1:], blank], axis=1)


def shift_cols(x, by):
    lane = lax.broadcasted_iota(jnp.int32, x.shape, 2)
    if by > 0:
        return jnp.where(lane == 0, 0.0, pltpu.roll(x, 1, 2))
    return jnp.where(lane == x.shape[2] - 1, 0.0, pltpu.roll(x, x.shape[2] - 1, 2))


def transport_kernel(
    inc_top, inc_own, inc_bot, top_ref, con_own, bot_ref, obs_own, inn_own, dep_ref, adj_ref
):
    halo = inc_top.shape[1]
    con_top, con_bot = [r[...].reshape((-1,) + inc_top.shape) for r in (top_ref, bot_ref)]
    rows = inc_own.shape[1]
    join = lambda a, b, c: jnp.concatenate([a, b, c], axis=1)
    state = join(inc_top[...], inc_own[...], inc_bot[...])

    def coeffs(step):
        c = [
            join(con_top[4 * step + k], con_own[4 * step + k], con_bot[4 * step + k]) for k in range(4)
        ]
        return c, 1.0 - (c[0] + c[1] + c[2] + c[3])

    for step in range(STEPS):
        c, center = coeffs(step)
        state = (
            center * state
            + c[0] * shift_rows(state, 1)
            + c[1] * shift_rows(state, -1)
            + c[2] * shift_cols(state, 1)
            + c[3] * shift_cols(state, -1)
        )
    weight = join(con_top[4 * STEPS], obs_own[...], con_bot[4 * STEPS])
    target = join(con_top[4 * STEPS + 1], inn_own[...], con_bot[4 * STEPS + 1])
    state = weight * (state - target)
    dep_ref[...] = state[:, halo : halo + rows]
    for step in range(STEPS - 1, -1, -1):
        c, center = coeffs(step)
        state = (
            center * state
            + shift_rows(c[0] * state, -1)
            + shift_rows(c[1] * state, 1)
            + shift_cols(c[2] * state, -1)
            + shift_cols(c[3] * state, 1)
        )
    adj_ref[...] = state[:, halo : halo + rows]


def transport(inc, con, obs_weight, innovation, used):
    shape = jax.ShapeDtypeStruct(obs_weight.shape, F32)
    whole = lambda a: pl.BlockSpec(a.shape, lambda i: (0,) * a.ndim)
    tail = con[0].shape[0] - used
    part = pl.BlockSpec(
        (pl.Element(tail), pl.Element(con[0].shape[1]), pl.Element(con[0].shape[2])), lambda i: (used, 0, 0)
    )
    return pl.pallas_call(
        transport_kernel,
        grid=(1,),
        in_specs=[whole(a) for a in inc] + [part, whole(con[1]), part, whole(obs_weight), whole(innovation)],
        out_specs=(whole(obs_weight), whole(obs_weight)),
        out_shape=(shape, shape),
        cost_estimate=pl.CostEstimate(flops=10**8, bytes_accessed=3 * 2**20, transcendentals=0),
        name="transport",
        compiler_params=pltpu.CompilerParams(vmem_limit_bytes=16 * MIB),
    )(*inc, *con, obs_weight, innovation)


def beside(block, dim, depth, axis="region"):
    count = lax.axis_size(axis)
    forward = [(i, i + 1) for i in range(count - 1)]
    backward = [(b, a) for a, b in forward]
    extent = block.shape[dim]
    low = lax.ppermute(lax.slice_in_dim(block, extent - depth, extent, axis=dim), axis, forward)
    high = lax.ppermute(lax.slice_in_dim(block, 0, depth, axis=dim), axis, backward)
    return low, high


def shards(controls, perturbations, assignment, courant, innovation, obs_weight):
    fields, levels, rows, cols = controls.shape
    planes = lax.axis_size("member")
    plane = lax.axis_index("member")
    regions = lax.axis_size("region")
    halo = 2 * STEPS

    col_basis, forward, backward, scale = diffusion_tables(rows, cols)
    tables = (
        jnp.asarray(col_basis),
        jnp.asarray(forward),
        jnp.asarray(backward),
        jnp.asarray(scale),
    )

    span = levels // PARTS
    partial_sums = [member_sums(assignment, perturbations, p, span, fields) for p in range(PARTS)]

    flat = courant.reshape((4 * STEPS,) + courant.shape[2:])

    def message(low):
        cut = lambda a, dim, depth: lax.slice_in_dim(
            a, *((0, depth) if low else (rows - depth, rows)), axis=dim
        )
        edge = [cut(flat, 2, halo), cut(obs_weight, 1, halo)[None], cut(innovation, 1, halo)[None]]
        return jnp.concatenate(
            [cut(controls, 2, PASSES).reshape(-1, TILE, cols)] + [e.reshape(-1, TILE, cols) for e in edge]
        )

    ahead = [(i, i + 1) for i in range(regions - 1)]
    top = lax.ppermute(message(False), "region", ahead)
    bot = lax.ppermute(message(True), "region", [(j, i) for i, j in ahead])
    used = fields * levels * PASSES // TILE
    smoothed = smooth(top, controls, bot, tables)

    up = [None] * PARTS
    down = [None] * PARTS
    for t in range(planes - 1):
        targets = jnp.clip(
            jnp.stack([plane + (planes - 1) - t, plane - (planes - 1) + t]), 0, planes - 1
        )
        for p in range(PARTS):
            whole, rise, fall = partial_sums[p]
            if t > 0:
                rise, fall = forward_sums(targets, whole, up[p], down[p])
            up[p] = lax.ppermute(rise, "member", [(i, i + 1) for i in range(t + 1)])
            down[p] = lax.ppermute(
                fall, "member", [(planes - 1 - i, planes - 2 - i) for i in range(t + 1)]
            )
    finished = finish_sums(
        plane[None], [whole for whole, _, _ in partial_sums], up, down, smoothed, planes
    )
    sums, partial = finished[:PARTS], finished[PARTS:]
    turn = lambda k: [(i, (i + k) % planes) for i in range(planes)]
    increment = partial[0]
    for k in range(1, planes):
        increment = increment + lax.ppermute(partial[k], "member", turn(k))
    inc_top, inc_bot = beside(increment, 1, halo)
    sums_ext = []
    for p in range(PARTS):
        sums_top, sums_bot = beside(sums[p], 2, PASSES)
        sums_ext += [sums_top, sums[p], sums_bot]
    departure, adjoint = transport(
        (inc_top, increment, inc_bot), (top, flat, bot), obs_weight, innovation, used
    )
    gathered = [adjoint]
    for k in range(1, planes):
        gathered.append(lax.ppermute(adjoint, "member", turn(k)))
    full = jnp.concatenate(gathered, axis=0)
    adj_top, adj_bot = beside(full, 1, PASSES)
    gradient = gradient_of(planes, controls, sums_ext, (adj_top, full, adj_bot), tables)
    return (gradient, departure)


def solution(mesh):
    return jax.shard_map(
        shards,
        mesh=mesh,
        in_specs=(
            P("member", None, "region", None),
            P("member", None, "region", None),
            P(),
            P(None, None, "member", "region", None),
            P("member", "region", None),
            P("member", "region", None),
        ),
        out_specs=(P("member", None, "region", None), P("member", "region", None)),
        check_vma=False,
    )
```
